32 devices in a mesh: row: 8 (over z, x), col: 4 (over y, core).
Axes of the slice: x: 2, y: 2, z: 4, core: 2. Of those that a mesh axis runs over, the one named last changes fastest.
Arguments:
- t2_amps: bfloat16 [16384, 49152], P('row', 'col'), may hold values from -0.5 to 0.5
- l2_amps: bfloat16 [256, 49152], P('row', 'col'), may hold values from -0.02734375 to 0.02734375
Outputs:
- ladder: bfloat16 [256, 49152], P('row', 'col')
The draws below stay inside these ranges and needn't reach their ends.
All inputs are finite; a program needn't handle non-finite values.
Results may differ from the reference program's by a relative error of at most 0.0044.
Values may be sent and summed in bfloat16 or wider, within the bound.
A program may use at most 128 MiB of HBM per device.

```python
import jax
import jax.numpy as jnp

O = 128
OO = 16384
PV = 49152
KL = 256


def block_levels(own_key, shape, shards, low, largest):
    def one(position, parts):
        draws = jax.random.uniform(jax.random.fold_in(jax.random.fold_in(own_key, 6), position), (parts,), jnp.float32, low / len(shards), largest / len(shards))
        return jnp.repeat(jnp.exp(draws), shape[position] // parts).reshape((-1,) + (1,) * (len(shape) - position - 1))

    factor_of = one(*shards[0])
    for cut in shards[1:]:
        factor_of = factor_of * one(*cut)
    return factor_of


def gaussian(key, extent, width, most, cuts=(), kind=jnp.bfloat16):
    values = jax.random.normal(key, extent, jnp.float32) * width
    if len(cuts) > 0:
        values = block_levels(key, extent, cuts, -0.22, 0.18) * values
    return jnp.clip(values, min=-most, max=most).astype(kind)


def setup_inputs(seed: int = 0) -> dict:
    splits = jax.random.split(jax.random.key(seed), 3)
    return {
        "t2_amps": gaussian(splits[0], (OO, PV), O ** -0.5, 0.5, ((0, 8), (1, 4))),
        "l2_amps": gaussian(splits[1], (KL, PV), PV ** -0.5, 0.02734375, ((0, 8), (1, 4))),
    }


def reference(t2_amps, l2_amps):
    oooo = jnp.dot(t2_amps, l2_amps.T, preferred_element_type=jnp.float32)
    oooo_half = oooo.astype(jnp.bfloat16)
    ladder = jnp.dot(oooo_half.T, t2_amps, preferred_element_type=jnp.float32)
    return ladder.astype(jnp.bfloat16)
```

```python
import functools

import jax
import jax.numpy as jnp
from jax import lax
from jax.experimental import pallas as pl
from jax.experimental.pallas import tpu as pltpu
from jax.sharding import PartitionSpec as P

MESH = pl.DeviceIdType.MESH
HALVES = 2
SLABS = 3
STREAMS = 4
CHUNKS_1 = 8
CHUNKS_2 = 8
BUFFERS = 3


def row_of(position, rows):
    upper = lax.div(position, rows // 2)
    return 2 * position + upper * (2 * rows - 1 - 4 * position)


def kernel(R, C, t2, l2, out, gath, acc, res, recv_a, sum_b, recv_b, half, half_t,
           rs_send, rs_recv, buf1, buf2, ag_ss, ag_rs, r_ss, r_rs, sem1, sem2,
           own_sem, a_sem, b_sem, c_sem, d_sem):
    IJ, AB = t2.shape
    H, Q, U = HALVES, SLABS, STREAMS
    KR = l2.shape[0] // H
    W = AB // Q
    WM = W // U
    n_short = R // 2 - 1
    TS = U * (R - 1) // 2
    AGS = H * Q
    chips = C // 2
    hij = IJ // 2
    bij = hij // chips
    rows1 = IJ // CHUNKS_1
    cols2 = W // CHUNKS_2

    my_row = lax.axis_index("row")
    my_col = lax.axis_index("col")
    a0, b0 = lax.div(my_row, 2), lax.rem(my_row, 2)
    me = a0 + b0 * (R - 1 - 2 * a0)
    ring = [row_of(lax.rem(me + 1, R), R), row_of(lax.rem(me + R - 1, R), R)]
    core = lax.rem(my_col, 2)
    chip = lax.div(my_col, 2)
    sibling = my_col + 1 - 2 * core

    def peer(d):
        return 2 * lax.rem(chip + d, chips) + core

    def block_row(offset):
        return pl.multiple_of(row_of(lax.rem(me + offset + 2 * R, R), R) * KR, KR)

    def dma1(c):
        a, i = lax.div(c, CHUNKS_1), lax.rem(c, CHUNKS_1)
        slot = lax.rem(c, BUFFERS)
        return pltpu.make_async_copy(
            t2.at[pl.ds(pl.multiple_of(i * rows1, rows1), rows1),
                  pl.ds(pl.multiple_of(lax.rem(a, Q) * W, W), W)],
            buf1.at[slot], sem1.at[slot])

    def dma2(c):
        slot = lax.rem(c, BUFFERS)
        k = lax.rem(c, Q * CHUNKS_2)
        return pltpu.make_async_copy(
            t2.at[:, pl.ds(pl.multiple_of(k * cols2, cols2), cols2)],
            buf2.at[slot], sem2.at[slot])

    def own(g):
        return pltpu.make_async_copy(
            l2.at[pl.ds(g * KR, KR), :], gath.at[g, pl.ds(block_row(0), KR), :],
            own_sem.at[g])

    for g in range(H):
        own(g).start()

    barrier = pltpu.get_barrier_semaphore()
    for r in ring:
        pl.semaphore_signal(barrier, inc=1, device_id=(r, my_col), device_id_type=MESH)
    pl.semaphore_signal(barrier, inc=1, device_id=(my_row, sibling), device_id_type=MESH)
    for d in range(1, chips):
        pl.semaphore_signal(barrier, inc=1, device_id=(my_row, peer(d)), device_id_type=MESH)
    pl.semaphore_wait(barrier, 2 + chips)

    for c in range(BUFFERS):
        dma1(jnp.int32(c)).start()
    for g in range(H):
        own(g).wait()

    def split(t):
        h = lax.div(t, U)
        last = lax.div(h, n_short)
        v = lax.rem(t, U) * (1 + last)
        return h, v

    def stream(v, d):
        return v if d == 0 else v + 1 - 2 * lax.rem(v, 2)

    def hops(v):
        return n_short + 1 - lax.rem(v, 2)

    def last_tick(v):
        odd = lax.rem(v, 2)
        return odd * ((n_short - 1) * U + v) + (1 - odd) * (n_short * U + lax.div(v, 2))

    def ag_copy(a, t, d):
        g, q = lax.div(a, Q), lax.rem(a, Q)
        h, v = split(t)
        u = stream(v, d)
        off = -h if d == 0 else h
        view = gath.at[g, pl.ds(block_row(off), KR),
                       pl.ds(pl.multiple_of(q * W + u * WM, WM), WM)]
        return pltpu.make_async_remote_copy(
            src_ref=view, dst_ref=view, send_sem=ag_ss.at[d, a, t], recv_sem=ag_rs.at[d, a, t],
            device_id=(ring[d], my_col), device_id_type=MESH)

    def ag_recv(a, t, d):
        g, q = lax.div(a, Q), lax.rem(a, Q)
        h, v = split(t)
        u = stream(v, d)
        off = -(h + 1) if d == 0 else h + 1
        view = gath.at[g, pl.ds(block_row(off), KR),
                       pl.ds(pl.multiple_of(q * W + u * WM, WM), WM)]
        return pltpu.make_async_remote_copy(
            src_ref=view, dst_ref=view, send_sem=ag_ss.at[d, a, t], recv_sem=ag_rs.at[d, a, t],
            device_id=(ring[d], my_col), device_id_type=MESH)

    def rs_copy(b, t, d):
        return pltpu.make_async_remote_copy(
            src_ref=rs_send.at[d, b, t], dst_ref=rs_recv.at[d, b, t],
            send_sem=r_ss.at[d, b, t], recv_sem=r_rs.at[d, b, t],
            device_id=(ring[d], my_col), device_id_type=MESH)

    def ag_tick(a, t):
        h, v = split(t)
        for d in range(2):
            @pl.when(h > 0)
            def _():
                ag_recv(a, t - U + (v - lax.rem(t, U)), d).wait_recv()
            ag_copy(a, t, d).start()

            @pl.when(a > 0)
            def _():
                ag_copy(a - 1, t, d).wait_send()

    def ag_finish(a):
        def one(v, _):
            for d in range(2):
                ag_recv(a, last_tick(v), d).wait_recv()
            return 0
        lax.fori_loop(0, U, one, 0)

    def rs_part(b, offset, u):
        return res[lax.rem(b, 2), pl.ds(block_row(offset), KR),
                   pl.ds(pl.multiple_of(u * WM, WM), WM)]

    def rs_tick(b, t):
        h, v = split(t)
        for d in range(2):
            u = stream(v, d)
            off = hops(v) - h
            off = off if d == 0 else -off

            @pl.when(h == 0)
            def _():
                rs_send[d, b, t] = rs_part(b, off, u).astype(jnp.bfloat16)

            @pl.when(h > 0)
            def _():
                before = t - U + (v - lax.rem(t, U))
                rs_copy(b, before, d).wait_recv()
                rs_send[d, b, t] = (
                    rs_part(b, off, u) + rs_recv[d, b, before].astype(jnp.float32)
                ).astype(jnp.bfloat16)
            rs_copy(b, t, d).start()

            @pl.when(b > 0)
            def _():
                rs_copy(b - 1, t, d).wait_send()

    def rs_finish(b):
        g, q = lax.div(b, Q), lax.rem(b, Q)

        def one(u, _):
            w = u + 1 - 2 * lax.rem(u, 2)
            rs_copy(b, last_tick(u), 0).wait_recv()
            rs_copy(b, last_tick(w), 1).wait_recv()
            total = (rs_part(b, 0, u) + rs_recv[0, b, last_tick(u)].astype(jnp.float32)
                     + rs_recv[1, b, last_tick(w)].astype(jnp.float32))
            out[pl.ds(pl.multiple_of(g * KR, KR), KR),
                pl.ds(pl.multiple_of(q * W + u * WM, WM), WM)] = total.astype(jnp.bfloat16)
            return 0
        lax.fori_loop(0, U, one, 0)

    def phase1(a, i):
        c = a * CHUNKS_1 + i
        g, q = lax.div(a, Q), lax.rem(a, Q)
        dma1(c).wait()
        part = lax.dot_general(
            buf1[lax.rem(c, BUFFERS)],
            gath[g, :, pl.ds(pl.multiple_of(q * W, W), W)],
            (((1,), (1,)), ((), ())), preferred_element_type=jnp.float32)
        where = pl.ds(pl.multiple_of(i * rows1, rows1), rows1)

        @pl.when(q == 0)
        def _():
            acc[g, where, :] = part

        @pl.when(q > 0)
        def _():
            acc[g, where, :] += part

        @pl.when(c + BUFFERS < AGS * CHUNKS_1)
        def _():
            dma1(c + BUFFERS).start()

    def phase2(b, i):
        c = b * CHUNKS_2 + i
        dma2(c).wait()
        res[lax.rem(b, 2), :, pl.ds(pl.multiple_of(i * cols2, cols2), cols2)] = jnp.dot(
            half_t[lax.div(b, Q)], buf2[lax.rem(c, BUFFERS)],
            preferred_element_type=jnp.float32)

        @pl.when(c + BUFFERS < AGS * CHUNKS_2)
        def _():
            dma2(c + BUFFERS).start()

    mine = pl.multiple_of(core * hij, hij)
    other = pl.multiple_of((1 - core) * hij, hij)
    my_block = pl.multiple_of(chip * bij, bij)

    def copy_a(g):
        return pltpu.make_async_remote_copy(
            src_ref=acc.at[g, pl.ds(other, hij), :], dst_ref=recv_a.at[g],
            send_sem=a_sem.at[0, g], recv_sem=a_sem.at[1, g],
            device_id=(my_row, sibling), device_id_type=MESH)

    def copy_b(g, d):
        return pltpu.make_async_remote_copy(
            src_ref=sum_b.at[g, pl.ds(pl.multiple_of(lax.rem(chip + d, chips) * bij, bij), bij), :],
            dst_ref=recv_b.at[g, d - 1],
            send_sem=b_sem.at[0, g, d - 1], recv_sem=b_sem.at[1, g, d - 1],
            device_id=(my_row, peer(d)), device_id_type=MESH)

    def copy_c(g, d, sender):
        view = half.at[g, pl.ds(pl.multiple_of(mine + sender * bij, bij), bij), :]
        return pltpu.make_async_remote_copy(
            src_ref=view, dst_ref=view,
            send_sem=c_sem.at[0, g, d - 1], recv_sem=c_sem.at[1, g, d - 1],
            device_id=(my_row, peer(d)), device_id_type=MESH)

    def copy_d(g, where):
        view = half.at[g, pl.ds(where, hij), :]
        return pltpu.make_async_remote_copy(
            src_ref=view, dst_ref=view, send_sem=d_sem.at[0, g], recv_sem=d_sem.at[1, g],
            device_id=(my_row, sibling), device_id_type=MESH)

    def stage_a(g):
        copy_a(g).start()

    def stage_b(g):
        copy_a(g).wait_recv()
        sum_b[g] = acc[g, pl.ds(mine, hij), :] + recv_a[g]
        for d in range(1, chips):
            copy_b(g, d).start()

    def stage_c(g):
        total = sum_b[g, pl.ds(my_block, bij), :]
        for d in range(1, chips):
            copy_b(g, d).wait_recv()
            total = total + recv_b[g, d - 1]
        half[g, pl.ds(pl.multiple_of(mine + my_block, bij), bij), :] = total.astype(jnp.bfloat16)
        for d in range(1, chips):
            copy_c(g, d, chip).start()

    def stage_d(g):
        for d in range(1, chips):
            copy_c(g, d, lax.rem(chip + chips - d, chips)).wait_recv()
        copy_d(g, mine).start()

    def stage_e(g):
        copy_d(g, other).wait_recv()

        step = 256

        def turn(i, _):
            at = pl.multiple_of(i * step, step)
            half_t[g, :, pl.ds(at, step)] = (
                half[g, pl.ds(at, step), :].astype(jnp.float32).T.astype(jnp.bfloat16))
            return 0
        lax.fori_loop(0, IJ // step, turn, 0)
        copy_a(g).wait_send()
        copy_d(g, mine).wait_send()
        for d in range(1, chips):
            copy_b(g, d).wait_send()
            copy_c(g, d, chip).wait_send()

    first1 = U
    first2 = TS - CHUNKS_2
    begin = first1 + CHUNKS_1
    finish = (Q - 1) * TS + first2 - 1 if Q > 1 else TS
    room = finish - begin
    events = [
        (begin, stage_a),
        (begin + 1, stage_b),
        (begin + 1 + (room - 2) * 6 // 10, stage_c),
        (begin + 1 + (room - 2) * 6 // 10 + (room - 2) * 4 // 10, stage_d),
        (finish, stage_e),
    ]

    def body(T, _):
        s, t = lax.div(T, TS), lax.rem(T, TS)

        @pl.when(s < AGS)
        def _():
            ag_tick(s, t)

        @pl.when(s >= AGS)
        def _():
            rs_tick(s - AGS, t)

        @pl.when((t == U - 1) & (s > 0) & (s <= AGS))
        def _():
            ag_finish(s - 1)

        @pl.when((t == U - 1) & (s > AGS))
        def _():
            rs_finish(s - 1 - AGS)

        @pl.when(T == TS)
        def _():
            for c in range(BUFFERS):
                dma2(jnp.int32(c)).start()

        @pl.when((s > 0) & (s <= AGS) & (t >= first1) & (t < first1 + CHUNKS_1))
        def _():
            phase1(s - 1, t - first1)

        for when, stage in events:
            since = T - when
            g = lax.div(since, Q * TS) - 1
            @pl.when((since >= Q * TS) & (lax.rem(since, Q * TS) == 0) & (g < H))
            def _():
                stage(g)

        @pl.when((s >= AGS - 1) & (s < 2 * AGS - 1) & (t >= first2))
        def _():
            phase2(s - (AGS - 1), t - first2)
        return 0

    lax.fori_loop(0, 2 * AGS * TS, body, 0)
    rs_finish(jnp.int32(AGS - 1))

    def drain(t, _):
        for d in range(2):
            ag_copy(AGS - 1, t, d).wait_send()
            rs_copy(AGS - 1, t, d).wait_send()
        return 0
    lax.fori_loop(0, TS, drain, 0)


def on_device(R, C, t2_amps, l2_amps):
    IJ, AB = t2_amps.shape
    H, Q, U = HALVES, SLABS, STREAMS
    KR = l2_amps.shape[0] // H
    K = KR * R
    W = AB // Q
    WM = W // U
    TS = U * (R - 1) // 2
    S = H * Q
    chips = C // 2
    hij = IJ // 2
    dma = pltpu.SemaphoreType.DMA
    return pl.pallas_call(
        functools.partial(kernel, R, C),
        out_shape=jax.ShapeDtypeStruct(l2_amps.shape, jnp.bfloat16),
        in_specs=[pl.BlockSpec(memory_space=pl.ANY)] * 2,
        out_specs=pl.BlockSpec(memory_space=pltpu.VMEM),
        scratch_shapes=[
            pltpu.VMEM((H, K, AB), jnp.bfloat16),
            pltpu.VMEM((H, IJ, K), jnp.float32),
            pltpu.VMEM((2, K, W), jnp.float32),
            pltpu.VMEM((H, hij, K), jnp.float32),
            pltpu.VMEM((H, hij, K), jnp.float32),
            pltpu.VMEM((H, chips - 1, hij // chips, K), jnp.float32),
            pltpu.VMEM((H, IJ, K), jnp.bfloat16),
            pltpu.VMEM((H, K, IJ), jnp.bfloat16),
            pltpu.VMEM((2, S, TS, KR, WM), jnp.bfloat16),
            pltpu.VMEM((2, S, TS, KR, WM), jnp.bfloat16),
            pltpu.VMEM((BUFFERS, IJ // CHUNKS_1, W), jnp.bfloat16),
            pltpu.VMEM((BUFFERS, IJ, W // CHUNKS_2), jnp.bfloat16),
            dma((2, S, TS)), dma((2, S, TS)), dma((2, S, TS)), dma((2, S, TS)),
            dma((BUFFERS,)), dma((BUFFERS,)), dma((H,)),
            dma((2, H)), dma((2, H, chips - 1)), dma((2, H, chips - 1)), dma((2, H)),
        ],
        compiler_params=pltpu.CompilerParams(
            collective_id=0, has_side_effects=True, vmem_limit_bytes=67000000),
    )(t2_amps, l2_amps)


def solution(mesh):
    R, C = mesh.shape["row"], mesh.shape["col"]
    return jax.shard_map(
        functools.partial(on_device, R, C),
        mesh=mesh,
        in_specs=(P("row", "col"), P("row", "col")),
        out_specs=P("row", "col"),
        check_vma=False,
    )
```

```python
import functools

import jax
import jax.numpy as jnp
from jax import lax
from jax.experimental import pallas as pl
from jax.experimental.pallas import tpu as pltpu
from jax.sharding import PartitionSpec as P

MESH = pl.DeviceIdType.MESH
HALVES = 2
SLABS = 2
STREAMS = 4
CHUNKS_1 = 8
CHUNKS_2 = 6
BUFFERS = 3


def row_of(position, rows):
    upper = lax.div(position, rows // 2)
    return 2 * position + upper * (2 * rows - 1 - 4 * position)


def kernel(R, C, t2, l2, out, gath, acc, res, recv_a, sum_b, recv_b, half, half_t,
           rs_send, rs_recv, buf1, buf2, ag_ss, ag_rs, r_ss, r_rs, sem1, sem2,
           own_sem, a_sem, b_sem, c_sem, d_sem):
    IJ, AB = t2.shape
    H, Q, U = HALVES, SLABS, STREAMS
    KR = l2.shape[0] // H
    W = AB // Q
    WM = W // U
    n_short = R // 2 - 1
    TS = U * (R - 1) // 2
    AGS = H * Q
    chips = C // 2
    hij = IJ // 2
    bij = hij // chips
    rows1 = IJ // CHUNKS_1
    cols2 = W // CHUNKS_2

    my_row = lax.axis_index("row")
    my_col = lax.axis_index("col")
    a0, b0 = lax.div(my_row, 2), lax.rem(my_row, 2)
    me = a0 + b0 * (R - 1 - 2 * a0)
    ring = [row_of(lax.rem(me + 1, R), R), row_of(lax.rem(me + R - 1, R), R)]
    core = lax.rem(my_col, 2)
    chip = lax.div(my_col, 2)
    sibling = my_col + 1 - 2 * core

    def peer(d):
        return 2 * lax.rem(chip + d, chips) + core

    def block_row(offset):
        return pl.multiple_of(row_of(lax.rem(me + offset + 2 * R, R), R) * KR, KR)

    def dma1(c):
        a, i = lax.div(c, CHUNKS_1), lax.rem(c, CHUNKS_1)
        slot = lax.rem(c, BUFFERS)
        return pltpu.make_async_copy(
            t2.at[pl.ds(pl.multiple_of(i * rows1, rows1), rows1),
                  pl.ds(pl.multiple_of(lax.rem(a, Q) * W, W), W)],
            buf1.at[slot], sem1.at[slot])

    def dma2(c):
        slot = lax.rem(c, BUFFERS)
        k = lax.rem(c, Q * CHUNKS_2)
        return pltpu.make_async_copy(
            t2.at[:, pl.ds(pl.multiple_of(k * cols2, cols2), cols2)],
            buf2.at[slot], sem2.at[slot])

    def own(g):
        return pltpu.make_async_copy(
            l2.at[pl.ds(g * KR, KR), :], gath.at[g, pl.ds(block_row(0), KR), :],
            own_sem.at[g])

    for g in range(H):
        own(g).start()

    barrier = pltpu.get_barrier_semaphore()
    for r in ring:
        pl.semaphore_signal(barrier, inc=1, device_id=(r, my_col), device_id_type=MESH)
    pl.semaphore_signal(barrier, inc=1, device_id=(my_row, sibling), device_id_type=MESH)
    for d in range(1, chips):
        pl.semaphore_signal(barrier, inc=1, device_id=(my_row, peer(d)), device_id_type=MESH)
    pl.semaphore_wait(barrier, 2 + chips)

    for c in range(BUFFERS):
        dma1(jnp.int32(c)).start()
    for g in range(H):
        own(g).wait()

    def split(t):
        h = lax.div(t, U)
        last = lax.div(h, n_short)
        v = lax.rem(t, U) * (1 + last)
        return h, v

    def stream(v, d):
        return v if d == 0 else v + 1 - 2 * lax.rem(v, 2)

    def hops(v):
        return n_short + 1 - lax.rem(v, 2)

    def last_tick(v):
        odd = lax.rem(v, 2)
        return odd * ((n_short - 1) * U + v) + (1 - odd) * (n_short * U + lax.div(v, 2))

    def ag_copy(a, t, d):
        g, q = lax.div(a, Q), lax.rem(a, Q)
        h, v = split(t)
        u = stream(v, d)
        off = -h if d == 0 else h
        view = gath.at[g, pl.ds(block_row(off), KR),
                       pl.ds(pl.multiple_of(q * W + u * WM, WM), WM)]
        return pltpu.make_async_remote_copy(
            src_ref=view, dst_ref=view, send_sem=ag_ss.at[d, a, t], recv_sem=ag_rs.at[d, a, t],
            device_id=(ring[d], my_col), device_id_type=MESH)

    def ag_recv(a, t, d):
        g, q = lax.div(a, Q), lax.rem(a, Q)
        h, v = split(t)
        u = stream(v, d)
        off = -(h + 1) if d == 0 else h + 1
        view = gath.at[g, pl.ds(block_row(off), KR),
                       pl.ds(pl.multiple_of(q * W + u * WM, WM), WM)]
        return pltpu.make_async_remote_copy(
            src_ref=view, dst_ref=view, send_sem=ag_ss.at[d, a, t], recv_sem=ag_rs.at[d, a, t],
            device_id=(ring[d], my_col), device_id_type=MESH)

    def rs_copy(b, t, d):
        return pltpu.make_async_remote_copy(
            src_ref=rs_send.at[d, b, t], dst_ref=rs_recv.at[d, b, t],
            send_sem=r_ss.at[d, b, t], recv_sem=r_rs.at[d, b, t],
            device_id=(ring[d], my_col), device_id_type=MESH)

    def ag_tick(a, t):
        h, v = split(t)
        for d in range(2):
            @pl.when(h > 0)
            def _():
                ag_recv(a, t - U + (v - lax.rem(t, U)), d).wait_recv()
            ag_copy(a, t, d).start()

            @pl.when(a > 0)
            def _():
                ag_copy(a - 1, t, d).wait_send()

    def ag_finish(a):
        def one(v, _):
            for d in range(2):
                ag_recv(a, last_tick(v), d).wait_recv()
            return 0
        lax.fori_loop(0, U, one, 0)

    def rs_part(b, offset, u):
        return res[lax.rem(b, 2), pl.ds(block_row(offset), KR),
                   pl.ds(pl.multiple_of(u * WM, WM), WM)]

    def rs_tick(b, t):
        h, v = split(t)
        for d in range(2):
            u = stream(v, d)
            off = hops(v) - h
            off = off if d == 0 else -off

            @pl.when(h == 0)
            def _():
                rs_send[d, b, t] = rs_part(b, off, u).astype(jnp.bfloat16)

            @pl.when(h > 0)
            def _():
                before = t - U + (v - lax.rem(t, U))
                rs_copy(b, before, d).wait_recv()
                rs_send[d, b, t] = (
                    rs_part(b, off, u) + rs_recv[d, b, before].astype(jnp.float32)
                ).astype(jnp.bfloat16)
            rs_copy(b, t, d).start()

            @pl.when(b > 0)
            def _():
                rs_copy(b - 1, t, d).wait_send()

    def rs_finish(b):
        g, q = lax.div(b, Q), lax.rem(b, Q)

        def one(u, _):
            w = u + 1 - 2 * lax.rem(u, 2)
            rs_copy(b, last_tick(u), 0).wait_recv()
            rs_copy(b, last_tick(w), 1).wait_recv()
            total = (rs_part(b, 0, u) + rs_recv[0, b, last_tick(u)].astype(jnp.float32)
                     + rs_recv[1, b, last_tick(w)].astype(jnp.float32))
            out[pl.ds(pl.multiple_of(g * KR, KR), KR),
                pl.ds(pl.multiple_of(q * W + u * WM, WM), WM)] = total.astype(jnp.bfloat16)
            return 0
        lax.fori_loop(0, U, one, 0)

    def phase1(a, i):
        c = a * CHUNKS_1 + i
        g, q = lax.div(a, Q), lax.rem(a, Q)
        dma1(c).wait()
        part = lax.dot_general(
            buf1[lax.rem(c, BUFFERS)],
            gath[g, :, pl.ds(pl.multiple_of(q * W, W), W)],
            (((1,), (1,)), ((), ())), preferred_element_type=jnp.float32)
        where = pl.ds(pl.multiple_of(i * rows1, rows1), rows1)

        @pl.when(q == 0)
        def _():
            acc[g, where, :] = part

        @pl.when(q > 0)
        def _():
            acc[g, where, :] += part

        @pl.when(c + BUFFERS < AGS * CHUNKS_1)
        def _():
            dma1(c + BUFFERS).start()

    def phase2(b, i):
        c = b * CHUNKS_2 + i
        dma2(c).wait()
        res[lax.rem(b, 2), :, pl.ds(pl.multiple_of(i * cols2, cols2), cols2)] = jnp.dot(
            half_t[lax.div(b, Q)], buf2[lax.rem(c, BUFFERS)],
            preferred_element_type=jnp.float32)

        @pl.when(c + BUFFERS < AGS * CHUNKS_2)
        def _():
            dma2(c + BUFFERS).start()

    mine = pl.multiple_of(core * hij, hij)
    other = pl.multiple_of((1 - core) * hij, hij)
    my_block = pl.multiple_of(chip * bij, bij)

    def copy_a(g):
        return pltpu.make_async_remote_copy(
            src_ref=acc.at[g, pl.ds(other, hij), :], dst_ref=recv_a.at[g],
            send_sem=a_sem.at[0, g], recv_sem=a_sem.at[1, g],
            device_id=(my_row, sibling), device_id_type=MESH)

    def copy_b(g, d):
        return pltpu.make_async_remote_copy(
            src_ref=sum_b.at[g, pl.ds(pl.multiple_of(lax.rem(chip + d, chips) * bij, bij), bij), :],
            dst_ref=recv_b.at[g, d - 1],
            send_sem=b_sem.at[0, g, d - 1], recv_sem=b_sem.at[1, g, d - 1],
            device_id=(my_row, peer(d)), device_id_type=MESH)

    def copy_c(g, d, sender):
        view = half.at[g, pl.ds(pl.multiple_of(mine + sender * bij, bij), bij), :]
        return pltpu.make_async_remote_copy(
            src_ref=view, dst_ref=view,
            send_sem=c_sem.at[0, g, d - 1], recv_sem=c_sem.at[1, g, d - 1],
            device_id=(my_row, peer(d)), device_id_type=MESH)

    def copy_d(g, where):
        view = half.at[g, pl.ds(where, hij), :]
        return pltpu.make_async_remote_copy(
            src_ref=view, dst_ref=view, send_sem=d_sem.at[0, g], recv_sem=d_sem.at[1, g],
            device_id=(my_row, sibling), device_id_type=MESH)

    def stage_a(g):
        copy_a(g).start()

    def stage_b(g):
        copy_a(g).wait_recv()
        sum_b[g] = acc[g, pl.ds(mine, hij), :] + recv_a[g]
        for d in range(1, chips):
            copy_b(g, d).start()

    def stage_c(g):
        total = sum_b[g, pl.ds(my_block, bij), :]
        for d in range(1, chips):
            copy_b(g, d).wait_recv()
            total = total + recv_b[g, d - 1]
        half[g, pl.ds(pl.multiple_of(mine + my_block, bij), bij), :] = total.astype(jnp.bfloat16)
        for d in range(1, chips):
            copy_c(g, d, chip).start()

    def stage_d(g):
        for d in range(1, chips):
            copy_c(g, d, lax.rem(chip + chips - d, chips)).wait_recv()
        copy_d(g, mine).start()

    def stage_e(g):
        copy_d(g, other).wait_recv()

        step = 256

        def turn(i, _):
            at = pl.multiple_of(i * step, step)
            half_t[g, :, pl.ds(at, step)] = (
                half[g, pl.ds(at, step), :].astype(jnp.float32).T.astype(jnp.bfloat16))
            return 0
        lax.fori_loop(0, IJ // step, turn, 0)
        copy_a(g).wait_send()
        copy_d(g, mine).wait_send()
        for d in range(1, chips):
            copy_b(g, d).wait_send()
            copy_c(g, d, chip).wait_send()

    first1 = U
    first2 = TS - CHUNKS_2
    begin = first1 + CHUNKS_1
    finish = (Q - 1) * TS + first2 - 1 if Q > 1 else TS
    room = finish - begin
    events = [
        (begin, stage_a),
        (begin + 1, stage_b),
        (begin + 1 + (room - 2) * 6 // 10, stage_c),
        (begin + 1 + (room - 2) * 6 // 10 + (room - 2) * 4 // 10, stage_d),
        (finish, stage_e),
    ]

    def body(T, _):
        s, t = lax.div(T, TS), lax.rem(T, TS)

        @pl.when(s < AGS)
        def _():
            ag_tick(s, t)

        @pl.when(s >= AGS)
        def _():
            rs_tick(s - AGS, t)

        @pl.when((t == U - 1) & (s > 0) & (s <= AGS))
        def _():
            ag_finish(s - 1)

        @pl.when((t == U - 1) & (s > AGS))
        def _():
            rs_finish(s - 1 - AGS)

        @pl.when(T == TS)
        def _():
            for c in range(BUFFERS):
                dma2(jnp.int32(c)).start()

        @pl.when((s > 0) & (s <= AGS) & (t >= first1) & (t < first1 + CHUNKS_1))
        def _():
            phase1(s - 1, t - first1)

        for when, stage in events:
            since = T - when
            g = lax.div(since, Q * TS) - 1
            @pl.when((since >= Q * TS) & (lax.rem(since, Q * TS) == 0) & (g < H))
            def _():
                stage(g)

        @pl.when((s >= AGS - 1) & (s < 2 * AGS - 1) & (t >= first2))
        def _():
            phase2(s - (AGS - 1), t - first2)
        return 0

    lax.fori_loop(0, 2 * AGS * TS, body, 0)
    rs_finish(jnp.int32(AGS - 1))

    def drain(t, _):
        for d in range(2):
            ag_copy(AGS - 1, t, d).wait_send()
            rs_copy(AGS - 1, t, d).wait_send()
        return 0
    lax.fori_loop(0, TS, drain, 0)


def on_device(R, C, t2_amps, l2_amps):
    IJ, AB = t2_amps.shape
    H, Q, U = HALVES, SLABS, STREAMS
    KR = l2_amps.shape[0] // H
    K = KR * R
    W = AB // Q
    WM = W // U
    TS = U * (R - 1) // 2
    S = H * Q
    chips = C // 2
    hij = IJ // 2
    dma = pltpu.SemaphoreType.DMA
    return pl.pallas_call(
        functools.partial(kernel, R, C),
        out_shape=jax.ShapeDtypeStruct(l2_amps.shape, jnp.bfloat16),
        in_specs=[pl.BlockSpec(memory_space=pl.ANY)] * 2,
        out_specs=pl.BlockSpec(memory_space=pltpu.VMEM),
        scratch_shapes=[
            pltpu.VMEM((H, K, AB), jnp.bfloat16),
            pltpu.VMEM((H, IJ, K), jnp.float32),
            pltpu.VMEM((2, K, W), jnp.float32),
            pltpu.VMEM((H, hij, K), jnp.float32),
            pltpu.VMEM((H, hij, K), jnp.float32),
            pltpu.VMEM((H, chips - 1, hij // chips, K), jnp.float32),
            pltpu.VMEM((H, IJ, K), jnp.bfloat16),
            pltpu.VMEM((H, K, IJ), jnp.bfloat16),
            pltpu.VMEM((2, S, TS, KR, WM), jnp.bfloat16),
            pltpu.VMEM((2, S, TS, KR, WM), jnp.bfloat16),
            pltpu.VMEM((BUFFERS, IJ // CHUNKS_1, W), jnp.bfloat16),
            pltpu.VMEM((BUFFERS, IJ, W // CHUNKS_2), jnp.bfloat16),
            dma((2, S, TS)), dma((2, S, TS)), dma((2, S, TS)), dma((2, S, TS)),
            dma((BUFFERS,)), dma((BUFFERS,)), dma((H,)),
            dma((2, H)), dma((2, H, chips - 1)), dma((2, H, chips - 1)), dma((2, H)),
        ],
        compiler_params=pltpu.CompilerParams(
            collective_id=0, has_side_effects=True, vmem_limit_bytes=67000000),
    )(t2_amps, l2_amps)


def solution(mesh):
    R, C = mesh.shape["row"], mesh.shape["col"]
    return jax.shard_map(
        functools.partial(on_device, R, C),
        mesh=mesh,
        in_specs=(P("row", "col"), P("row", "col")),
        out_specs=P("row", "col"),
        check_vma=False,
    )
```
